32 devices in a mesh: pool: 4 (over z), fft: 8 (over y, x, core).
Axes of the slice: x: 2, y: 2, z: 4, core: 2. Of those that a mesh axis runs over, the one named last changes fastest.
Arguments:
- orbitals: bfloat16 [4, 2, 1, 160, 25600], P('pool', None, None, 'fft'), may hold values from -6 to 6
- stick_map: int32 [16000], replicated, may hold values from -1 to 25599, as said below
- kpoint_grid: int32 [4, 3], replicated, may hold values from 0 to 3, as said below
Outputs:
- exchange_action: bfloat16 [4, 2, 1, 160, 25600], P('pool', None, None, 'fft')
The draws below stay inside these ranges and needn't reach their ends.
Inputs may be any that keep to these rules, and one draw needn't show every extreme that they name: `stick_map`: entries other than -1 are distinct columns. Slots come in blocks of 2000 per index of fft; in each block at least half of the slots are live, and in every draw some block has all 2000 live. `kpoint_grid`: rows are distinct.
All inputs are finite; a program needn't handle non-finite values.
Results may differ from the reference program's by a relative error of at most 0.011.
Values may be sent and summed in bfloat16 or wider, within the bound.
No kernel may reach another device: no remote copies, remote signals or barrier semaphores. Data moves between devices by JAX's collectives and lax.ppermute only.
A program may use at most 64 MiB of HBM per device.

```python
import math
import jax
import jax.numpy as jnp
from jax import lax

NG = 160
BANDS = 1
KMESH = 4
KPOINTS = 4
STICKS_DEV = 2000
STICKS_ALL = 16000


def draw_stick_map(key, part):
    devices = STICKS_ALL // STICKS_DEV
    key_counts = jax.random.fold_in(key, 11)
    key_full = jax.random.fold_in(key, 12)
    key_order = jax.random.fold_in(key, 13)
    counts = jax.random.randint(key_counts, (devices,), STICKS_DEV // 2, STICKS_DEV + 1)
    full_device = jax.random.randint(key_full, (), 0, devices)
    device_ids = jnp.arange(devices, dtype=jnp.int32)
    counts = jnp.where(device_ids == full_device, STICKS_DEV, counts).astype(jnp.int32)
    offsets = jnp.cumsum(counts) - counts
    shuffled = jax.random.permutation(key_order, NG * NG).astype(jnp.int32)
    column_x = shuffled % NG
    column_y = shuffled // NG
    signed_x = jnp.where(column_x >= NG // 2, column_x - NG, column_x)
    signed_y = jnp.where(column_y >= NG // 2, column_y - NG, column_y)
    outside = (signed_x * signed_x + signed_y * signed_y > NG // 2 * (NG // 2)).astype(jnp.int32)
    ordering = jnp.argsort(outside, stable=True)
    columns = shuffled[ordering]
    slot_ids = jnp.arange(STICKS_DEV, dtype=jnp.int32)
    positions = offsets[:, None] + slot_ids[None, :]
    positions = jnp.minimum(positions, NG * NG - 1)
    chosen = columns[positions]
    filled = jnp.where(slot_ids[None, :] < counts[:, None], chosen, -1)
    return filled.reshape(STICKS_ALL).astype(jnp.int32)


def draw_kpoint_grid(key, part):
    picked = jax.random.permutation(jax.random.fold_in(key, 21), KMESH * KMESH * KMESH)[:KPOINTS].astype(jnp.int32)
    first = picked // (KMESH * KMESH)
    second = picked // KMESH % KMESH
    third = picked % KMESH
    return jnp.stack([first, second, third], axis=1).astype(jnp.int32)


def steps_of(key, extent, split, low, largest):
    def one(position, shards_of):
        heights = jax.random.uniform(jax.random.fold_in(jax.random.fold_in(key, 6), position), (shards_of,), jnp.float32, low / len(split), largest / len(split))
        return jnp.repeat(jnp.exp(heights), extent[position] // shards_of).reshape((-1,) + (1,) * (len(extent) - position - 1))

    level = one(*split[0])
    for cut in split[1:]:
        level = level * one(*cut)
    return level


def noise(stream_key, shape, spread, bound, cuts=(), kind=jnp.bfloat16):
    values = jax.random.normal(stream_key, shape, jnp.float32) * spread
    if len(cuts) > 0:
        values = steps_of(stream_key, shape, cuts, -0.22, 0.18) * values
    return jnp.clip(values, min=-bound, max=bound).astype(kind)


def setup_inputs(seed: int = 0) -> dict:
    seeds = jax.random.split(jax.random.key(seed), 4)
    return {
        "orbitals": noise(seeds[0], (KPOINTS, 2, BANDS, NG, NG * NG), 1.0, 6.0, ((0, 4), (3, 8))),
        "stick_map": draw_stick_map(jax.random.fold_in(seeds[3], 71), 0),
        "kpoint_grid": draw_kpoint_grid(jax.random.fold_in(seeds[3], 71), 0),
    }


SPACING_BOHR = 0.1875
SCREENING = 0.106


def dft_table(grid_size, orientation):
    positions = jnp.arange(grid_size, dtype=jnp.int32)
    product = (positions[:, None] * positions[None, :]) % grid_size
    angle = product.astype(jnp.float32) * (2.0 * math.pi / grid_size)
    cosine = jnp.cos(angle)
    sine = orientation * jnp.sin(angle)
    upper = jnp.stack([cosine, sine], axis=1)
    lower = jnp.stack([-sine, cosine], axis=1)
    return jnp.stack([upper, lower], axis=0).astype(jnp.bfloat16)


def signed(frequency, grid_size):
    return jnp.where(frequency >= grid_size // 2, frequency - grid_size, frequency)


def kernel_table(columns, shift_q, grid_size):
    live_slot = columns >= 0
    column_ids = jnp.where(live_slot, columns, 0)
    freq_x = signed(column_ids % grid_size, grid_size)
    freq_y = signed(column_ids // grid_size, grid_size)
    freq_z = signed(jnp.arange(grid_size, dtype=jnp.int32), grid_size)
    radius = grid_size // 2
    inside = (freq_x * freq_x + freq_y * freq_y)[None, :] + (freq_z * freq_z)[:, None] <= radius * radius
    inside = jnp.logical_and(inside, live_slot[None, :])
    wave_x = freq_x.astype(jnp.float32) + shift_q[0]
    wave_y = freq_y.astype(jnp.float32) + shift_q[1]
    wave_z = freq_z.astype(jnp.float32) + shift_q[2]
    square = (wave_z * wave_z)[:, None] + (wave_x * wave_x + wave_y * wave_y)[None, :]
    cell = SPACING_BOHR * grid_size
    exponent = (math.pi * math.pi) * square / (cell * cell * SCREENING * SCREENING)
    weights = (cell * cell / math.pi) * (-jnp.expm1(-exponent)) / square / (float(grid_size) ** 3)
    return jnp.where(inside, weights, 0.0).astype(jnp.float32)


def momentum(kpoint_grid, pool_rank, pool_count):
    pool_rows = jnp.arange(pool_count, dtype=jnp.int32)
    earlier = (pool_rank + pool_count - 1) % pool_count
    current = jnp.sum(jnp.where((pool_rows == pool_rank)[:, None], kpoint_grid, 0), axis=0)
    previous = jnp.sum(jnp.where((pool_rows == earlier)[:, None], kpoint_grid, 0), axis=0)
    return (current - previous).astype(jnp.float32) / KMESH


def pair_density(own_bands, received):
    band_count = own_bands.shape[1]
    real_own = own_bands[0].astype(jnp.float32)[:, None]
    imag_own = own_bands[1].astype(jnp.float32)[:, None]
    real_recv = received[0].astype(jnp.float32)[None]
    imag_recv = received[1].astype(jnp.float32)[None]
    real_part = real_recv * real_own + imag_recv * imag_own
    imag_part = real_recv * imag_own - imag_recv * real_own
    stacked = jnp.stack([real_part, imag_part], axis=2)
    return stacked.reshape((band_count * band_count, 2) + own_bands.shape[2:]).astype(jnp.bfloat16)


def action_of(received, field):
    band_count = received.shape[1]
    field = field.reshape((band_count, band_count) + field.shape[1:])
    real_recv = received[0].astype(jnp.float32)[None]
    imag_recv = received[1].astype(jnp.float32)[None]
    real_field = field[:, :, 0]
    imag_field = field[:, :, 1]
    real_part = -jnp.sum(real_recv * real_field - imag_recv * imag_field, axis=1)
    imag_part = -jnp.sum(real_recv * imag_field + imag_recv * real_field, axis=1)
    return jnp.stack([real_part, imag_part], axis=0).astype(jnp.bfloat16)


def apply_table(data, table, form):
    return jnp.einsum(form, data.astype(jnp.float32), table.astype(jnp.float32), precision=lax.Precision.HIGHEST)


def column_pass(picked, weights, forward, backward):
    spectrum = apply_table(picked, forward, "pczs,czdk->pdks")
    scaled = (spectrum * weights).astype(jnp.bfloat16)
    return apply_table(scaled, backward, "pczs,czdk->pdks").astype(jnp.bfloat16)


def reference(orbitals, stick_map, kpoint_grid):
    pool_count = orbitals.shape[0]
    grid_size = orbitals.shape[3]
    orbitals = orbitals.reshape(orbitals.shape[:4] + (grid_size, grid_size))
    forward = dft_table(grid_size, -1.0)
    backward = dft_table(grid_size, 1.0)
    live_slot = stick_map >= 0
    column_ids = jnp.where(live_slot, stick_map, 0).astype(jnp.int32)

    def one_pool(pool_rank):
        own_bands = lax.dynamic_index_in_dim(orbitals, pool_rank, 0, keepdims=False)
        earlier = ((pool_rank + pool_count - 1) % pool_count).astype(jnp.int32)
        received = lax.dynamic_index_in_dim(orbitals, earlier, 0, keepdims=False)
        density = pair_density(own_bands, received)
        along_x = apply_table(density, forward, "pczyx,cxek->pezyk").astype(jnp.bfloat16)
        along_y = apply_table(along_x, forward, "pczyx,cyek->pezkx").astype(jnp.bfloat16)
        flattened = along_y.reshape(along_y.shape[:3] + (grid_size * grid_size,))
        picked = jnp.where(live_slot, jnp.take(flattened, column_ids, axis=3), 0).astype(jnp.bfloat16)
        weights = kernel_table(stick_map, momentum(kpoint_grid, pool_rank, pool_count), grid_size)
        returned = column_pass(picked, weights, forward, backward)
        merged = jnp.zeros_like(flattened).at[:, :, :, column_ids].add(jnp.where(live_slot, returned, 0).astype(jnp.bfloat16))
        back_y = apply_table(merged.reshape(along_y.shape), backward, "pczkx,ckey->pezyx").astype(jnp.bfloat16)
        field = apply_table(back_y, backward, "pczyk,ckex->pezyx")
        result = action_of(received, field)
        return result.reshape(result.shape[:3] + (grid_size * grid_size,))

    return lax.map(one_pool, jnp.arange(pool_count, dtype=jnp.int32))
```

```python
import math

import jax
import jax.numpy as jnp
from jax import lax
from jax.sharding import PartitionSpec as P

NG = 160
KMESH = 4


SPACING_BOHR = 0.1875
SCREENING = 0.106


def shifted(value, axis, steps):
    count = lax.axis_size(axis)
    pairs = [(source, (source + steps) % count) for source in range(count)]
    return lax.ppermute(value, axis, pairs)


def dft_table(grid_size, orientation):
    positions = jnp.arange(grid_size, dtype=jnp.int32)
    product = positions[:, None] * positions[None, :] % grid_size
    angle = product.astype(jnp.float32) * (2.0 * math.pi / grid_size)
    cosine = jnp.cos(angle)
    sine = orientation * jnp.sin(angle)
    upper = jnp.stack([cosine, sine], axis=1)
    lower = jnp.stack([-sine, cosine], axis=1)
    return jnp.stack([upper, lower], axis=0).astype(jnp.bfloat16)


def signed(frequency, grid_size):
    return jnp.where(frequency >= grid_size // 2, frequency - grid_size, frequency)


def kernel_table(columns, shift_q, grid_size):
    live_slot = columns >= 0
    column_ids = jnp.where(live_slot, columns, 0)
    freq_x = signed(column_ids % grid_size, grid_size)
    freq_y = signed(column_ids // grid_size, grid_size)
    freq_z = signed(jnp.arange(grid_size, dtype=jnp.int32), grid_size)
    radius = grid_size // 2
    inside = (freq_x * freq_x + freq_y * freq_y)[None, :] + (freq_z * freq_z)[
        :, None
    ] <= radius * radius
    inside = jnp.logical_and(inside, live_slot[None, :])
    wave_x = freq_x.astype(jnp.float32) + shift_q[0]
    wave_y = freq_y.astype(jnp.float32) + shift_q[1]
    wave_z = freq_z.astype(jnp.float32) + shift_q[2]
    square = (wave_z * wave_z)[:, None] + (wave_x * wave_x + wave_y * wave_y)[None, :]
    cell = SPACING_BOHR * grid_size
    exponent = math.pi * math.pi * square / (cell * cell * SCREENING * SCREENING)
    weights = cell * cell / math.pi * -jnp.expm1(-exponent) / square / float(grid_size) ** 3
    return jnp.where(inside, weights, 0.0)


def momentum(kpoint_grid, pool_rank, pool_count):
    pool_rows = jnp.arange(pool_count, dtype=jnp.int32)
    earlier = (pool_rank + pool_count - 1) % pool_count
    current = jnp.sum(jnp.where((pool_rows == pool_rank)[:, None], kpoint_grid, 0), axis=0)
    previous = jnp.sum(jnp.where((pool_rows == earlier)[:, None], kpoint_grid, 0), axis=0)
    return (current - previous).astype(jnp.float32) / KMESH


def pair_density(own_bands, received):
    band_count = own_bands.shape[1]
    real_own = own_bands[0].astype(jnp.float32)[:, None]
    imag_own = own_bands[1].astype(jnp.float32)[:, None]
    real_recv = received[0].astype(jnp.float32)[None]
    imag_recv = received[1].astype(jnp.float32)[None]
    real_part = real_recv * real_own + imag_recv * imag_own
    imag_part = real_recv * imag_own - imag_recv * real_own
    stacked = jnp.stack([real_part, imag_part], axis=2)
    return stacked.reshape((band_count * band_count, 2) + own_bands.shape[2:]).astype(jnp.bfloat16)


def action_of(received, field):
    band_count = received.shape[1]
    field = field.reshape((band_count, band_count) + field.shape[1:])
    real_recv = received[0].astype(jnp.float32)[None]
    imag_recv = received[1].astype(jnp.float32)[None]
    real_field = field[:, :, 0]
    imag_field = field[:, :, 1]
    real_part = -jnp.sum(real_recv * real_field - imag_recv * imag_field, axis=1)
    imag_part = -jnp.sum(real_recv * imag_field + imag_recv * real_field, axis=1)
    return jnp.stack([real_part, imag_part], axis=0).astype(jnp.bfloat16)


def apply_table(data, table, form):
    return jnp.einsum(form, data, table, preferred_element_type=jnp.float32)


def column_pass(picked, weights, forward, backward):
    spectrum = apply_table(picked, forward, "pczs,czdk->pdks")
    scaled = (spectrum * weights).astype(jnp.bfloat16)
    return apply_table(scaled, backward, "pczs,czdk->pdks").astype(jnp.bfloat16)


def present_columns(stick_map, first_row, row_count, grid_size):
    rows = first_row + jnp.arange(row_count, dtype=jnp.int32)
    column_y = jnp.where(stick_map >= 0, stick_map // grid_size, -1)
    column_x = stick_map % grid_size
    hit_y = (rows[:, None] == column_y[None, :]).astype(jnp.bfloat16)
    hit_x = (jnp.arange(grid_size, dtype=jnp.int32)[:, None] == column_x[None, :]).astype(jnp.bfloat16)
    counts = lax.dot_general(hit_y, hit_x, (((1,), (1,)), ((), ())), preferred_element_type=jnp.float32)
    return counts > 0.5


def local(orbitals, stick_map, kpoint_grid):
    grid_size = NG
    moved = shifted(orbitals, "pool", 1)
    own_bands = orbitals[0].reshape(orbitals.shape[1:4] + (grid_size, grid_size))
    received = moved[0].reshape(orbitals.shape[1:4] + (grid_size, grid_size))
    fft_count = lax.axis_size("fft")
    fft_rank = lax.axis_index("fft")
    pool_count = lax.axis_size("pool")
    pool_rank = lax.axis_index("pool")
    shift_q = momentum(kpoint_grid, pool_rank, pool_count)
    forward = dft_table(grid_size, -1.0)
    backward = dft_table(grid_size, 1.0)
    column_share = grid_size * grid_size // fft_count
    rows_share = grid_size // fft_count
    share_ids = fft_rank * column_share + jnp.arange(column_share, dtype=jnp.int32)
    own_present = present_columns(stick_map, fft_rank * rows_share, rows_share, grid_size).reshape(column_share)
    weights = kernel_table(jnp.where(own_present, share_ids, -1), shift_q, grid_size)

    def potential(pair_block):
        along_x = apply_table(pair_block, forward, "pczyx,cxek->pezyk").astype(jnp.bfloat16)
        along_y = apply_table(along_x, forward, "pczyx,cyek->pezkx").astype(jnp.bfloat16)
        piece_block = lax.all_to_all(along_y, "fft", split_axis=3, concat_axis=2, tiled=True)
        flat_piece = piece_block.reshape(piece_block.shape[:3] + (column_share,))
        scaled_back = column_pass(flat_piece, weights, forward, backward).reshape(piece_block.shape)
        spectrum = lax.all_to_all(scaled_back, "fft", split_axis=2, concat_axis=3, tiled=True)
        back_y = apply_table(spectrum, backward, "pczkx,ckey->pezyx").astype(jnp.bfloat16)
        return apply_table(back_y, backward, "pczyk,ckex->pezyx")

    density = pair_density(own_bands, received)
    field = lax.map(lambda single_pair: potential(single_pair[None])[0], density)
    result = action_of(received, field)
    return result.reshape((1,) + result.shape[:3] + (grid_size * grid_size,))


def solution(mesh):
    return jax.shard_map(
        local,
        mesh=mesh,
        in_specs=(P("pool", None, None, "fft", None), P(), P()),
        out_specs=P("pool", None, None, "fft", None),
        check_vma=False,
    )
```

```python
import functools
import math

import jax
import jax.numpy as jnp
import numpy as np
from jax import lax
from jax.experimental import pallas as pl
from jax.experimental.pallas import tpu as pltpu
from jax.sharding import PartitionSpec as P

NG = 160
KMESH = 4
LANES = 128


SPACING_BOHR = 0.1875
SCREENING = 0.106

GROUP = math.lcm(NG, LANES) // NG
TILES = GROUP * NG // LANES
GROUPS = NG // GROUP
ROWS = 2 * NG * NG // LANES
STEP = 2 * TILES
OUTER = NG - LANES
HALF = LANES // 2


def shifted(value, axis, steps):
    count = lax.axis_size(axis)
    pairs = [(source, (source + steps) % count) for source in range(count)]
    return lax.ppermute(value, axis, pairs)


def dft_table(grid_size, orientation):
    positions = np.arange(grid_size)
    angle = (positions[:, None] * positions[None, :] % grid_size) * (2.0 * np.pi / grid_size)
    cosine = np.cos(angle)
    sine = orientation * np.sin(angle)
    upper = np.stack([cosine, sine], axis=1)
    lower = np.stack([-sine, cosine], axis=1)
    return np.stack([upper, lower], axis=0)


def inner(table, axis):
    size = table.shape[axis]
    return np.concatenate(
        [np.take(table, range(HALF), axis), np.take(table, range(size - HALF, size), axis)], axis
    )


def outer(table, axis):
    return np.take(table, range(HALF, table.shape[axis] - HALF), axis)


def padded(table, axis, size):
    widths = [(0, 0)] * table.ndim
    widths[axis] = (0, size - table.shape[axis])
    return np.pad(table, widths)


def tables(fft_count):
    share = NG // fft_count
    fwd = dft_table(NG, -1.0)
    bwd = dft_table(NG, 1.0)
    full = 2 * NG
    x_fwd = np.concatenate(
        [inner(fwd, 3).reshape(2, NG, 2 * LANES), padded(outer(fwd, 3), 3, LANES).reshape(2, NG, 2 * LANES)], 2
    )
    x_bwd = np.concatenate(
        [inner(bwd, 1).reshape(2 * LANES, 2, NG), padded(outer(bwd, 1), 1, LANES).reshape(2 * LANES, 2, NG)], 0
    )
    split = fwd.reshape(2, GROUPS, GROUP, 2, fft_count, share)
    y_fwd = split.transpose(4, 3, 5, 0, 2, 1).reshape(full, full)
    y_fwd_side = inner(fwd.reshape(2, GROUPS, GROUP, 2, NG).transpose(0, 2, 1, 3, 4), 4).reshape(full, 2 * LANES)
    z_fwd = fwd.transpose(2, 3, 0, 1).reshape(full, full)
    z_bwd = bwd.reshape(2, NG, 2, fft_count, share).transpose(3, 2, 4, 0, 1).reshape(full, full)
    order = bwd.reshape(2, NG, 2, GROUPS, GROUP).transpose(2, 4, 3, 0, 1)
    y_bwd = order.reshape(full, full)
    y_bwd_side = inner(order, 4).reshape(full, 2 * LANES)
    cast = lambda t: jnp.asarray(t.astype(np.float32).astype(jnp.bfloat16))
    return [cast(t) for t in (x_fwd, x_bwd, y_fwd, y_fwd_side, z_fwd, z_bwd, y_bwd, y_bwd_side)]


def signed(frequency, grid_size):
    return jnp.where(frequency >= grid_size // 2, frequency - grid_size, frequency)


def kernel_table(column_x, column_y, live, shift_q, grid_size):
    freq_x = signed(column_x, grid_size)
    freq_y = signed(column_y, grid_size)
    freq_z = signed(jnp.arange(grid_size, dtype=jnp.int32), grid_size)
    radius = grid_size // 2
    inside = (freq_x * freq_x + freq_y * freq_y)[None, :] + (freq_z * freq_z)[:, None] <= radius * radius
    inside = jnp.logical_and(inside, live[None, :])
    wave_x = freq_x.astype(jnp.float32) + shift_q[0]
    wave_y = freq_y.astype(jnp.float32) + shift_q[1]
    wave_z = freq_z.astype(jnp.float32) + shift_q[2]
    square = (wave_z * wave_z)[:, None] + (wave_x * wave_x + wave_y * wave_y)[None, :]
    cell = SPACING_BOHR * grid_size
    exponent = math.pi * math.pi * square / (cell * cell * SCREENING * SCREENING)
    weights = cell * cell / math.pi * -jnp.expm1(-exponent) / square / float(grid_size) ** 3
    return jnp.where(inside, weights, 0.0)


def momentum(kpoint_grid, pool_rank, pool_count):
    pool_rows = jnp.arange(pool_count, dtype=jnp.int32)
    earlier = (pool_rank + pool_count - 1) % pool_count
    current = jnp.sum(jnp.where((pool_rows == pool_rank)[:, None], kpoint_grid, 0), axis=0)
    previous = jnp.sum(jnp.where((pool_rows == earlier)[:, None], kpoint_grid, 0), axis=0)
    return (current - previous).astype(jnp.float32) / KMESH


def one_hot(values, wanted):
    return (wanted[:, None] == values[None, :]).astype(jnp.bfloat16)


def column_weights(stick_map, kpoint_grid, fft_rank, share, side_share):
    pool_count = lax.axis_size("pool")
    shift_q = momentum(kpoint_grid, lax.axis_index("pool"), pool_count)
    lanes = jnp.arange(LANES, dtype=jnp.int32)
    inner_freq = jnp.where(lanes < HALF, lanes, lanes + OUTER)
    own_y = fft_rank * share + jnp.arange(share, dtype=jnp.int32)
    own_x = HALF + fft_rank * side_share + jnp.arange(side_share, dtype=jnp.int32)
    column_y = jnp.where(stick_map >= 0, stick_map // NG, -1)
    column_x = jnp.where(stick_map >= 0, stick_map % NG, -1)
    form = (((1,), (1,)), ((), ()))
    main = lax.dot_general(
        one_hot(column_y, own_y), one_hot(column_x, inner_freq), form, preferred_element_type=jnp.float32
    )
    side = lax.dot_general(
        one_hot(column_x, own_x), one_hot(column_y, inner_freq), form, preferred_element_type=jnp.float32
    )
    live = jnp.concatenate([main, side], axis=0).reshape(-1) > 0.5
    place = jnp.arange((share + side_share) * LANES, dtype=jnp.int32)
    row = place // LANES
    lane_freq = jnp.where(place % LANES < HALF, place % LANES, place % LANES + OUTER)
    is_main = row < share
    ids_x = jnp.where(is_main, lane_freq, HALF + fft_rank * side_share + row - share)
    ids_y = jnp.where(is_main, fft_rank * share + row, lane_freq)
    return kernel_table(ids_x, ids_y, live, shift_q, NG)


def dot(left, right, form=(((1,), (0,)), ((), ()))):
    return lax.dot_general(left, right, form, preferred_element_type=jnp.float32)


def pieces(ref, plane, tile, part):
    return ref[pl.ds(plane * ROWS + 2 * tile + part, GROUPS, stride=STEP), :]


def pairs_of(count):
    return [tuple(range(i, min(i + 2, count))) for i in range(0, count, 2)]


def forward_kernel(own_ref, recv_ref, x_ref, y_ref, side_ref, out_ref, own_f, recv_f, *, planes, fft_count):
    share = NG // fft_count
    side_share = OUTER // fft_count
    own_f[...] = own_ref[...].astype(jnp.float32)
    recv_f[...] = recv_ref[...].astype(jnp.float32)
    density = []
    for tile in range(TILES):
        real, imag = [], []
        for z in range(planes):
            ro, io = pieces(own_f, z, tile, 0), pieces(own_f, z, tile, 1)
            rr, ir = pieces(recv_f, z, tile, 0), pieces(recv_f, z, tile, 1)
            real.append(rr * ro + ir * io)
            imag.append(rr * io - ir * ro)
        density.append(
            (jnp.concatenate(real, 0).astype(jnp.bfloat16), jnp.concatenate(imag, 0).astype(jnp.bfloat16))
        )
    along_x = []
    for r in range(GROUP):
        left = jnp.concatenate([density[r][0], density[r + 1][0], density[r][1], density[r + 1][1]], axis=1)
        along_x.append(dot(left, x_ref[r]))

    def block(z, r, column):
        return along_x[r][z * GROUPS : (z + 1) * GROUPS, column * LANES : (column + 1) * LANES]

    def stacked(z, first):
        return jnp.concatenate([block(z, r, first + c) for c in range(2) for r in range(GROUP)], axis=0)

    for pair in pairs_of(planes):
        right = jnp.concatenate([stacked(z, 0) for z in pair], axis=1).astype(jnp.bfloat16)
        along_y = dot(y_ref[...], right)
        for n, z in enumerate(pair):
            for k in range(fft_count):
                out_ref[k, z, : 2 * share, :] = along_y[
                    2 * share * k : 2 * share * (k + 1), n * LANES : (n + 1) * LANES
                ].astype(jnp.bfloat16)
    side = stacked(0, 2)
    for z in range(1, planes):
        side = side + pltpu.roll(stacked(z, 2), z * OUTER, 1)
    side = side[:, : planes * OUTER].astype(jnp.bfloat16)
    side_y = dot(side, side_ref[...], (((0,), (0,)), ((), ())))
    for z in range(planes):
        for k in range(fft_count):
            row = z * OUTER + k * side_share
            out_ref[k, z, 2 * share :, :] = jnp.concatenate(
                [side_y[row : row + side_share, c * LANES : (c + 1) * LANES] for c in range(2)], axis=0
            ).astype(jnp.bfloat16)


def column_kernel(in_ref, weight_ref, fwd_ref, bwd_ref, out_ref, wide, *, fft_count):
    share = NG // fft_count
    side_share = OUTER // fft_count
    height = 2 * (share + side_share)
    wide[...] = in_ref[...].reshape(NG * height, LANES).astype(jnp.float32)

    def column(i):
        first = i if i < share else 2 * share + i - share
        jump = share if i < share else side_share
        return jnp.concatenate([wide[pl.ds(first + c * jump, NG, stride=height), :] for c in range(2)], axis=0)

    for pair in pairs_of(share + side_share):
        right = jnp.concatenate([column(i) for i in pair], axis=1).astype(jnp.bfloat16)
        spectrum = dot(fwd_ref[...], right)
        weight = weight_ref[:, pair[0] * LANES : (pair[-1] + 1) * LANES]
        scaled = jnp.concatenate([spectrum[:NG] * weight, spectrum[NG:] * weight], axis=0).astype(jnp.bfloat16)
        back = dot(bwd_ref[...], scaled)
        for n, i in enumerate(pair):
            for k in range(fft_count):
                out_ref[k, i, :, :] = back[
                    2 * share * k : 2 * share * (k + 1), n * LANES : (n + 1) * LANES
                ].astype(jnp.bfloat16)


def backward_kernel(
    in_ref, recv_ref, x_ref, y_ref, side_ref, out_ref, main_f, side_f, recv_f, out_f, *, planes, fft_count
):
    share = NG // fft_count
    side_share = OUTER // fft_count
    height = 2 * share

    @pl.when(pl.program_id(0) == 0)
    def _():
        for k in range(fft_count):
            main_f[pl.ds(k * share * height, share * height), :] = (
                in_ref[k, :share].reshape(share * height, LANES).astype(jnp.float32)
            )
            side_f[pl.ds(k * side_share * height, side_share * height), :] = (
                in_ref[k, share:].reshape(side_share * height, LANES).astype(jnp.float32)
            )

    recv_f[...] = recv_ref[...].astype(jnp.float32)
    base = pl.program_id(0) * planes

    def main_of(z):
        return jnp.concatenate(
            [main_f[pl.ds(base + z + c * share, NG, stride=height), :] for c in range(2)], axis=0
        )

    def side_of(z):
        return jnp.concatenate(
            [side_f[pl.ds(base + z + c * share, OUTER, stride=height), :] for c in range(2)], axis=1
        )

    back_y = []
    for pair in pairs_of(planes):
        right = jnp.concatenate([main_of(z) for z in pair], axis=1).astype(jnp.bfloat16)
        both = dot(y_ref[...], right)
        back_y += [both[:, n * LANES : (n + 1) * LANES] for n in range(len(pair))]
    packed = jnp.concatenate([side_of(z) for z in range(planes)], axis=0).astype(jnp.bfloat16)
    back_side = dot(side_ref[...], packed, (((1,), (1,)), ((), ())))
    if planes * OUTER < LANES:
        back_side = jnp.concatenate(
            [back_side, jnp.zeros((2 * NG, LANES - planes * OUTER), jnp.float32)], axis=1
        )
    turned = [back_side] + [pltpu.roll(back_side, LANES - z * OUTER, 1) for z in range(1, planes)]
    field = []
    for r in range(GROUP):
        rows = []
        for z in range(planes):
            parts = [v[c * NG + r * GROUPS : c * NG + (r + 1) * GROUPS] for v in (back_y[z], turned[z]) for c in range(2)]
            rows.append(jnp.concatenate(parts, axis=1))
        field.append(dot(jnp.concatenate(rows, axis=0).astype(jnp.bfloat16), x_ref[r]))
    for tile in range(TILES):
        values = []
        for c in range(2):
            value = None
            if tile < GROUP:
                value = field[tile][:, 2 * c * LANES : (2 * c + 1) * LANES]
            if tile > 0:
                late = field[tile - 1][:, (2 * c + 1) * LANES : (2 * c + 2) * LANES]
                value = late if value is None else value + late
            values.append(value)
        for z in range(planes):
            re, im = (v[z * GROUPS : (z + 1) * GROUPS] for v in values)
            rr, ir = pieces(recv_f, z, tile, 0), pieces(recv_f, z, tile, 1)
            out_f[pl.ds(z * ROWS + 2 * tile, GROUPS, stride=STEP), :] = ir * im - rr * re
            out_f[pl.ds(z * ROWS + 2 * tile + 1, GROUPS, stride=STEP), :] = -(rr * im + ir * re)
    out_ref[...] = out_f[...].astype(jnp.bfloat16)


def rows_of(orbitals):
    planes = orbitals.shape[3]
    split = orbitals.reshape(2, planes, NG * NG // LANES, LANES)
    return split.transpose(1, 2, 0, 3).reshape(planes * ROWS, LANES)


def whole(shape):
    return pl.BlockSpec(shape, lambda *_: (0,) * len(shape))


def x_windows(table, axis):
    placed = []
    for r in range(GROUP):
        first = r * (NG - LANES)
        widths = [(0, 0)] * table.ndim
        widths[axis] = (first, 2 * LANES - NG - first)
        placed.append(jnp.pad(table, widths).reshape(4 * LANES, 4 * LANES))
    return jnp.stack(placed)


def local(orbitals, stick_map, kpoint_grid):
    moved = shifted(orbitals, "pool", 1)
    planes_all = orbitals.shape[3]
    planes = GROUP if planes_all % GROUP == 0 else 1
    steps = planes_all // planes
    fft_count = lax.axis_size("fft")
    fft_rank = lax.axis_index("fft")
    share = NG // fft_count
    side_share = OUTER // fft_count
    columns = share + side_share
    x_fwd, x_bwd, y_fwd, y_fwd_side, z_fwd, z_bwd, y_bwd, y_bwd_side = tables(fft_count)
    x_fwd = x_windows(x_fwd, 1)
    x_bwd = x_windows(x_bwd, 2)
    weights = column_weights(stick_map, kpoint_grid, fft_rank, share, side_share)
    own = rows_of(orbitals)
    received = rows_of(moved)
    block = planes * ROWS
    row_spec = pl.BlockSpec((block, LANES), lambda s: (s, 0))
    params = pltpu.CompilerParams(vmem_limit_bytes=48 << 20)
    wide = lambda count: pltpu.VMEM((count, LANES), jnp.float32)
    spectrum = pl.pallas_call(
        functools.partial(forward_kernel, planes=planes, fft_count=fft_count),
        grid=(steps,),
        in_specs=[row_spec, row_spec, whole(x_fwd.shape), whole(y_fwd.shape), whole(y_fwd_side.shape)],
        out_specs=pl.BlockSpec((fft_count, planes, 2 * columns, LANES), lambda s: (0, s, 0, 0)),
        out_shape=jax.ShapeDtypeStruct((fft_count, planes_all, 2 * columns, LANES), jnp.bfloat16),
        scratch_shapes=[wide(block), wide(block)],
        compiler_params=params,
        name="density_xy",
    )(own, received, x_fwd, y_fwd, y_fwd_side)
    spectrum = lax.all_to_all(spectrum, "fft", 0, 0, tiled=True)
    scaled = pl.pallas_call(
        functools.partial(column_kernel, fft_count=fft_count),
        out_shape=jax.ShapeDtypeStruct((fft_count, columns, 2 * share, LANES), jnp.bfloat16),
        scratch_shapes=[wide(NG * 2 * columns)],
        compiler_params=params,
        name="columns",
    )(spectrum, weights, z_fwd, z_bwd)
    scaled = lax.all_to_all(scaled, "fft", 0, 0, tiled=True)
    result = pl.pallas_call(
        functools.partial(backward_kernel, planes=planes, fft_count=fft_count),
        grid=(steps,),
        in_specs=[whole(scaled.shape), row_spec, whole(x_bwd.shape), whole(y_bwd.shape), whole(y_bwd_side.shape)],
        out_specs=row_spec,
        out_shape=jax.ShapeDtypeStruct((planes_all * ROWS, LANES), jnp.bfloat16),
        scratch_shapes=[wide(NG * 2 * share), wide(OUTER * 2 * share), wide(block), wide(block)],
        compiler_params=params,
        name="yx_action",
    )(scaled, received, x_bwd, y_bwd, y_bwd_side)
    result = result.reshape(planes_all, NG * NG // LANES, 2, LANES).transpose(2, 0, 1, 3)
    return result.reshape(orbitals.shape)


def solution(mesh):
    return jax.shard_map(
        local,
        mesh=mesh,
        in_specs=(P("pool", None, None, "fft", None), P(), P()),
        out_specs=P("pool", None, None, "fft", None),
        check_vma=False,
    )
```

```python
import functools
import math

import jax
import jax.numpy as jnp
import numpy as np
from jax import lax
from jax.experimental import pallas as pl
from jax.experimental.pallas import tpu as pltpu
from jax.sharding import PartitionSpec as P

NG = 160
KMESH = 4
LANES = 128


SPACING_BOHR = 0.1875
SCREENING = 0.106

GROUP = math.lcm(NG, LANES) // NG
TILES = GROUP * NG // LANES
GROUPS = NG // GROUP
ROWS = 2 * NG * NG // LANES
STEP = 2 * TILES
OUTER = NG - LANES
HALF = LANES // 2


def shifted(value, axis, steps):
    count = lax.axis_size(axis)
    pairs = [(source, (source + steps) % count) for source in range(count)]
    return lax.ppermute(value, axis, pairs)


def dft_table(grid_size, orientation):
    positions = np.arange(grid_size)
    angle = (positions[:, None] * positions[None, :] % grid_size) * (2.0 * np.pi / grid_size)
    cosine = np.cos(angle)
    sine = orientation * np.sin(angle)
    upper = np.stack([cosine, sine], axis=1)
    lower = np.stack([-sine, cosine], axis=1)
    return np.stack([upper, lower], axis=0)


def inner(table, axis):
    size = table.shape[axis]
    return np.concatenate(
        [np.take(table, range(HALF), axis), np.take(table, range(size - HALF, size), axis)], axis
    )


def outer(table, axis):
    return np.take(table, range(HALF, table.shape[axis] - HALF), axis)


def padded(table, axis, size):
    widths = [(0, 0)] * table.ndim
    widths[axis] = (0, size - table.shape[axis])
    return np.pad(table, widths)


def tables(fft_count, back_planes, planes):
    share = NG // fft_count
    fwd = dft_table(NG, -1.0)
    bwd = dft_table(NG, 1.0)
    full = 2 * NG
    x_fwd = np.concatenate(
        [inner(fwd, 3).reshape(2, NG, 2 * LANES), padded(outer(fwd, 3), 3, LANES).reshape(2, NG, 2 * LANES)], 2
    )
    x_bwd = np.concatenate(
        [inner(bwd, 1).reshape(2 * LANES, 2, NG), padded(outer(bwd, 1), 1, LANES).reshape(2 * LANES, 2, NG)], 0
    )
    split = fwd.reshape(2, GROUPS, GROUP, 2, fft_count, share)
    y_fwd = split.transpose(4, 3, 5, 0, 2, 1).reshape(full, full)
    y_fwd_side = inner(fwd.reshape(2, GROUPS, GROUP, 2, NG).transpose(0, 2, 1, 3, 4), 4).reshape(full, 2 * LANES)
    z_fwd = fwd.reshape(2, fft_count, share // planes, planes, full)
    z_fwd = z_fwd.transpose(4, 0, 2, 1, 3).reshape(full, full)
    z_split = bwd.reshape(2, NG, 2, fft_count, share).transpose(3, 2, 4, 0, 1)
    edges = np.cumsum([0] + back_planes)
    z_bwd = np.concatenate([z_split[:, :, a:b].reshape(-1, full) for a, b in zip(edges[:-1], edges[1:])], 0)
    order = bwd.reshape(2, NG, 2, GROUPS, GROUP).transpose(2, 4, 3, 0, 1)
    y_bwd = order.reshape(full, full)
    y_bwd_side = inner(order, 4).reshape(full, 2 * LANES)
    cast = lambda t: jnp.asarray(t.astype(np.float32).astype(jnp.bfloat16))
    return [cast(t) for t in (x_fwd, x_bwd, y_fwd, y_fwd_side, z_fwd, z_bwd, y_bwd, y_bwd_side)]


def signed(frequency, grid_size):
    return jnp.where(frequency >= grid_size // 2, frequency - grid_size, frequency)


def kernel_table(column_x, column_y, live, shift_q, grid_size):
    freq_x = signed(column_x, grid_size)
    freq_y = signed(column_y, grid_size)
    freq_z = signed(jnp.arange(grid_size, dtype=jnp.int32), grid_size)
    radius = grid_size // 2
    inside = (freq_x * freq_x + freq_y * freq_y)[None, :] + (freq_z * freq_z)[:, None] <= radius * radius
    inside = jnp.logical_and(inside, live[None, :])
    wave_x = freq_x.astype(jnp.float32) + shift_q[0]
    wave_y = freq_y.astype(jnp.float32) + shift_q[1]
    wave_z = freq_z.astype(jnp.float32) + shift_q[2]
    square = (wave_z * wave_z)[:, None] + (wave_x * wave_x + wave_y * wave_y)[None, :]
    cell = SPACING_BOHR * grid_size
    exponent = math.pi * math.pi * square / (cell * cell * SCREENING * SCREENING)
    weights = cell * cell / math.pi * -jnp.expm1(-exponent) / square / float(grid_size) ** 3
    return jnp.where(inside, weights, 0.0)


def momentum(kpoint_grid, pool_rank, pool_count):
    pool_rows = jnp.arange(pool_count, dtype=jnp.int32)
    earlier = (pool_rank + pool_count - 1) % pool_count
    current = jnp.sum(jnp.where((pool_rows == pool_rank)[:, None], kpoint_grid, 0), axis=0)
    previous = jnp.sum(jnp.where((pool_rows == earlier)[:, None], kpoint_grid, 0), axis=0)
    return (current - previous).astype(jnp.float32) / KMESH


def one_hot(values, wanted):
    return (wanted[:, None] == values[None, :]).astype(jnp.bfloat16)


def column_weights(stick_map, kpoint_grid, fft_rank, share, side_share):
    pool_count = lax.axis_size("pool")
    shift_q = momentum(kpoint_grid, lax.axis_index("pool"), pool_count)
    lanes = jnp.arange(LANES, dtype=jnp.int32)
    inner_freq = jnp.where(lanes < HALF, lanes, lanes + OUTER)
    own_y = fft_rank * share + jnp.arange(share, dtype=jnp.int32)
    own_x = HALF + fft_rank * side_share + jnp.arange(side_share, dtype=jnp.int32)
    column_y = jnp.where(stick_map >= 0, stick_map // NG, -1)
    column_x = jnp.where(stick_map >= 0, stick_map % NG, -1)
    form = (((1,), (1,)), ((), ()))
    main = lax.dot_general(
        one_hot(column_y, own_y), one_hot(column_x, inner_freq), form, preferred_element_type=jnp.float32
    )
    side = lax.dot_general(
        one_hot(column_x, own_x), one_hot(column_y, inner_freq), form, preferred_element_type=jnp.float32
    )
    live = jnp.concatenate([main, side], axis=0).reshape(-1) > 0.5
    place = jnp.arange((share + side_share) * LANES, dtype=jnp.int32)
    row = place // LANES
    lane_freq = jnp.where(place % LANES < HALF, place % LANES, place % LANES + OUTER)
    is_main = row < share
    ids_x = jnp.where(is_main, lane_freq, HALF + fft_rank * side_share + row - share)
    ids_y = jnp.where(is_main, fft_rank * share + row, lane_freq)
    return kernel_table(ids_x, ids_y, live, shift_q, NG)


def dot(left, right, form=(((1,), (0,)), ((), ()))):
    return lax.dot_general(left, right, form, preferred_element_type=jnp.float32)


def pieces(ref, plane, tile, part):
    return ref[pl.ds(plane * ROWS + 2 * tile + part, GROUPS, stride=STEP), :]


def pairs_of(count):
    return [tuple(range(i, min(i + 2, count))) for i in range(0, count, 2)]


def forward_kernel(own_ref, recv_ref, x_ref, y_ref, side_ref, out_ref, own_f, recv_f, *, planes, fft_count):
    share = NG // fft_count
    side_share = OUTER // fft_count
    own_f[...] = own_ref[...].astype(jnp.float32)
    recv_f[...] = recv_ref[...].astype(jnp.float32)
    density = []
    for tile in range(TILES):
        real, imag = [], []
        for z in range(planes):
            ro, io = pieces(own_f, z, tile, 0), pieces(own_f, z, tile, 1)
            rr, ir = pieces(recv_f, z, tile, 0), pieces(recv_f, z, tile, 1)
            real.append(rr * ro + ir * io)
            imag.append(rr * io - ir * ro)
        density.append(
            (jnp.concatenate(real, 0).astype(jnp.bfloat16), jnp.concatenate(imag, 0).astype(jnp.bfloat16))
        )
    along_x = []
    for r in range(GROUP):
        left = jnp.concatenate([density[r][0], density[r + 1][0], density[r][1], density[r + 1][1]], axis=1)
        along_x.append(dot(left, x_ref[r]))

    def block(z, r, column):
        return along_x[r][z * GROUPS : (z + 1) * GROUPS, column * LANES : (column + 1) * LANES]

    def stacked(z, first):
        return jnp.concatenate([block(z, r, first + c) for c in range(2) for r in range(GROUP)], axis=0)

    for pair in pairs_of(planes):
        right = jnp.concatenate([stacked(z, 0) for z in pair], axis=1).astype(jnp.bfloat16)
        along_y = dot(y_ref[...], right)
        for n, z in enumerate(pair):
            for k in range(fft_count):
                out_ref[k, z, : 2 * share, :] = along_y[
                    2 * share * k : 2 * share * (k + 1), n * LANES : (n + 1) * LANES
                ].astype(jnp.bfloat16)
    side = stacked(0, 2)
    for z in range(1, planes):
        side = side + pltpu.roll(stacked(z, 2), z * OUTER, 1)
    side = side[:, : planes * OUTER].astype(jnp.bfloat16)
    side_y = dot(side, side_ref[...], (((0,), (0,)), ((), ())))
    for z in range(planes):
        for k in range(fft_count):
            row = z * OUTER + k * side_share
            out_ref[k, z, 2 * share :, :] = jnp.concatenate(
                [side_y[row : row + side_share, c * LANES : (c + 1) * LANES] for c in range(2)], axis=0
            ).astype(jnp.bfloat16)


def column_kernel(*refs, fft_count, steps, back_planes):
    in_refs = refs[:steps]
    weight_ref, fwd_ref, bwd_ref = refs[steps : steps + 3]
    out_refs = refs[steps + 3 : -1]
    wide = refs[-1]
    share = NG // fft_count
    side_share = OUTER // fft_count
    height = 2 * (share + side_share)
    rows = NG // steps * height
    for s, in_ref in enumerate(in_refs):
        wide[s * rows : (s + 1) * rows, :] = in_ref[...].reshape(rows, LANES).astype(jnp.float32)

    def column(i):
        first = i if i < share else 2 * share + i - share
        jump = share if i < share else side_share
        return jnp.concatenate([wide[pl.ds(first + c * jump, NG, stride=height), :] for c in range(2)], axis=0)

    for pair in pairs_of(share + side_share):
        right = jnp.concatenate([column(i) for i in pair], axis=1).astype(jnp.bfloat16)
        spectrum = dot(fwd_ref[...], right)
        weight = weight_ref[:, pair[0] * LANES : (pair[-1] + 1) * LANES]
        scaled = jnp.concatenate([spectrum[:NG] * weight, spectrum[NG:] * weight], axis=0).astype(jnp.bfloat16)
        back = dot(bwd_ref[...], scaled)
        for n, i in enumerate(pair):
            first = 0
            for out_ref, depth in zip(out_refs, back_planes):
                for k in range(fft_count):
                    out_ref[k, i, :, :] = back[first : first + 2 * depth, n * LANES : (n + 1) * LANES].astype(
                        jnp.bfloat16
                    )
                    first += 2 * depth


def backward_kernel(*refs, planes, depth, base, fft_count):
    in_ref, recv_ref, x_ref, y_ref, side_ref = refs[:5]
    out_ref, main_f, side_f, recv_f, out_f = refs[-5:]
    share = NG // fft_count
    side_share = OUTER // fft_count
    height = 2 * depth
    for k in range(fft_count):
        main_f[k * share * height : (k + 1) * share * height, :] = (
            in_ref[k, :share].reshape(share * height, LANES).astype(jnp.float32)
        )
        side_f[k * side_share * height : (k + 1) * side_share * height, :] = (
            in_ref[k, share:].reshape(side_share * height, LANES).astype(jnp.float32)
        )
    recv_f[...] = recv_ref[...].astype(jnp.float32)

    def main_of(z):
        return jnp.concatenate(
            [main_f[pl.ds(base + z + c * depth, NG, stride=height), :] for c in range(2)], axis=0
        )

    def side_of(z):
        return jnp.concatenate(
            [side_f[pl.ds(base + z + c * depth, OUTER, stride=height), :] for c in range(2)], axis=1
        )

    back_y = []
    for pair in pairs_of(planes):
        right = jnp.concatenate([main_of(z) for z in pair], axis=1).astype(jnp.bfloat16)
        both = dot(y_ref[...], right)
        back_y += [both[:, n * LANES : (n + 1) * LANES] for n in range(len(pair))]
    packed = jnp.concatenate([side_of(z) for z in range(planes)], axis=0).astype(jnp.bfloat16)
    back_side = dot(side_ref[...], packed, (((1,), (1,)), ((), ())))
    if planes * OUTER < LANES:
        back_side = jnp.concatenate(
            [back_side, jnp.zeros((2 * NG, LANES - planes * OUTER), jnp.float32)], axis=1
        )
    turned = [back_side] + [pltpu.roll(back_side, LANES - z * OUTER, 1) for z in range(1, planes)]
    field = []
    for r in range(GROUP):
        rows = []
        for z in range(planes):
            parts = [v[c * NG + r * GROUPS : c * NG + (r + 1) * GROUPS] for v in (back_y[z], turned[z]) for c in range(2)]
            rows.append(jnp.concatenate(parts, axis=1))
        field.append(dot(jnp.concatenate(rows, axis=0).astype(jnp.bfloat16), x_ref[r]))
    for tile in range(TILES):
        values = []
        for c in range(2):
            value = None
            if tile < GROUP:
                value = field[tile][:, 2 * c * LANES : (2 * c + 1) * LANES]
            if tile > 0:
                late = field[tile - 1][:, (2 * c + 1) * LANES : (2 * c + 2) * LANES]
                value = late if value is None else value + late
            values.append(value)
        for z in range(planes):
            re, im = (v[z * GROUPS : (z + 1) * GROUPS] for v in values)
            rr, ir = pieces(recv_f, z, tile, 0), pieces(recv_f, z, tile, 1)
            out_f[pl.ds(z * ROWS + 2 * tile, GROUPS, stride=STEP), :] = ir * im - rr * re
            out_f[pl.ds(z * ROWS + 2 * tile + 1, GROUPS, stride=STEP), :] = -(rr * im + ir * re)
    out_ref[...] = out_f[...].astype(jnp.bfloat16)


def rows_of(orbitals):
    planes = orbitals.shape[3]
    split = orbitals.reshape(2, planes, NG * NG // LANES, LANES)
    return split.transpose(1, 2, 0, 3).reshape(planes * ROWS, LANES)


def whole(shape):
    return pl.BlockSpec(shape, lambda *_: (0,) * len(shape))


def x_windows(table, axis):
    placed = []
    for r in range(GROUP):
        first = r * (NG - LANES)
        widths = [(0, 0)] * table.ndim
        widths[axis] = (first, 2 * LANES - NG - first)
        placed.append(jnp.pad(table, widths).reshape(4 * LANES, 4 * LANES))
    return jnp.stack(placed)


def chunk_planes(planes_all, planes):
    return [planes] * (planes_all // planes)


def local(orbitals, stick_map, kpoint_grid):
    planes_all = orbitals.shape[3]
    planes = GROUP if planes_all % GROUP == 0 else 1
    steps = planes_all // planes
    back_planes = chunk_planes(planes_all, planes)
    moved = [shifted(orbitals[:, :, :, s * planes : (s + 1) * planes], "pool", 1) for s in range(steps)]
    fft_count = lax.axis_size("fft")
    fft_rank = lax.axis_index("fft")
    share = NG // fft_count
    side_share = OUTER // fft_count
    columns = share + side_share
    x_fwd, x_bwd, y_fwd, y_fwd_side, z_fwd, z_bwd, y_bwd, y_bwd_side = tables(fft_count, back_planes, planes)
    x_fwd = x_windows(x_fwd, 1)
    x_bwd = x_windows(x_bwd, 2)
    weights = column_weights(stick_map, kpoint_grid, fft_rank, share, side_share)
    own = rows_of(orbitals)
    received = [rows_of(piece) for piece in moved]
    block = planes * ROWS
    row_spec = lambda s: pl.BlockSpec((block, LANES), lambda _: (s, 0))
    params = pltpu.CompilerParams(vmem_limit_bytes=48 << 20)
    wide = lambda count: pltpu.VMEM((count, LANES), jnp.float32)
    spectra = []
    for s in range(steps):
        spectrum = pl.pallas_call(
            functools.partial(forward_kernel, planes=planes, fft_count=fft_count),
            grid=(1,),
            in_specs=[row_spec(s), row_spec(0), whole(x_fwd.shape), whole(y_fwd.shape), whole(y_fwd_side.shape)],
            out_specs=whole((fft_count, planes, 2 * columns, LANES)),
            out_shape=jax.ShapeDtypeStruct((fft_count, planes, 2 * columns, LANES), jnp.bfloat16),
            scratch_shapes=[wide(block), wide(block)],
            compiler_params=params,
            name="density_xy",
        )(own, received[s], x_fwd, y_fwd, y_fwd_side)
        spectra.append(lax.all_to_all(spectrum, "fft", 0, 0, tiled=True))
    scaled = pl.pallas_call(
        functools.partial(column_kernel, fft_count=fft_count, steps=steps, back_planes=back_planes),
        out_shape=[
            jax.ShapeDtypeStruct((fft_count, columns, 2 * depth, LANES), jnp.bfloat16) for depth in back_planes
        ],
        scratch_shapes=[wide(NG * 2 * columns)],
        compiler_params=params,
        name="columns",
    )(*spectra, weights, z_fwd, z_bwd)
    returned = [lax.all_to_all(piece, "fft", 0, 0, tiled=True) for piece in scaled]
    result = None
    s = 0
    for piece, depth in zip(returned, back_planes):
        for base in range(0, depth, planes):
            inputs = [piece, received[s], x_bwd, y_bwd, y_bwd_side]
            specs = [whole(piece.shape), row_spec(0), whole(x_bwd.shape), whole(y_bwd.shape), whole(y_bwd_side.shape)]
            if s > 0:
                inputs.append(result)
                specs.append(pl.BlockSpec(memory_space=pl.ANY))
            result = pl.pallas_call(
                functools.partial(backward_kernel, planes=planes, depth=depth, base=base, fft_count=fft_count),
                grid=(1,),
                in_specs=specs,
                out_specs=row_spec(s),
                out_shape=jax.ShapeDtypeStruct((planes_all * ROWS, LANES), jnp.bfloat16),
                scratch_shapes=[wide(NG * 2 * depth), wide(OUTER * 2 * depth), wide(block), wide(block)],
                input_output_aliases={5: 0} if s > 0 else {},
                compiler_params=params,
                name="yx_action",
            )(*inputs)
            s += 1
    result = result.reshape(planes_all, NG * NG // LANES, 2, LANES).transpose(2, 0, 1, 3)
    return result.reshape(orbitals.shape)


def solution(mesh):
    return jax.shard_map(
        local,
        mesh=mesh,
        in_specs=(P("pool", None, None, "fft", None), P(), P()),
        out_specs=P("pool", None, None, "fft", None),
        check_vma=False,
    )
```

```python
import functools
import math

import jax
import jax.numpy as jnp
import numpy as np
from jax import lax
from jax.experimental import pallas as pl
from jax.experimental.pallas import tpu as pltpu
from jax.sharding import PartitionSpec as P


NG = 160
KMESH = 4
LANES = 128


SPACING_BOHR = 0.1875
SCREENING = 0.106

GROUP = math.lcm(NG, LANES) // NG
TILES = GROUP * NG // LANES
GROUPS = NG // GROUP
ROWS = 2 * NG * NG // LANES
STEP = 2 * TILES
OUTER = NG - LANES
HALF = LANES // 2


def shifted(value, axis, steps):
    count = lax.axis_size(axis)
    pairs = [(source, (source + steps) % count) for source in range(count)]
    return lax.ppermute(value, axis, pairs)


def dft_table(grid_size, orientation):
    positions = np.arange(grid_size)
    angle = (positions[:, None] * positions[None, :] % grid_size) * (2.0 * np.pi / grid_size)
    cosine = np.cos(angle)
    sine = orientation * np.sin(angle)
    upper = np.stack([cosine, sine], axis=1)
    lower = np.stack([-sine, cosine], axis=1)
    return np.stack([upper, lower], axis=0)


def inner(table, axis):
    size = table.shape[axis]
    return np.concatenate(
        [np.take(table, range(HALF), axis), np.take(table, range(size - HALF, size), axis)], axis
    )


def outer(table, axis):
    return np.take(table, range(HALF, table.shape[axis] - HALF), axis)


def met(table, axis, rank):
    count = table.shape[axis]
    bits = count.bit_length() - 1
    split = table.reshape(table.shape[:axis] + (2,) * bits + table.shape[axis + 1 :])
    for bit in range(bits):
        swapped = jnp.flip(split, axis + bits - 1 - bit)
        split = jnp.where((rank >> bit) & 1 == 1, swapped, split)
    return split.reshape(table.shape)


def tables(fft_count, rank, chunks):
    share = NG // fft_count
    side_share = OUTER // fft_count
    fwd = dft_table(NG, -1.0)
    bwd = dft_table(NG, 1.0)
    full = 2 * NG
    cast = lambda t: jnp.asarray(t.astype(np.float32).astype(jnp.bfloat16))
    side = met(cast(outer(fwd, 3).reshape(2, NG, 2, fft_count, side_share)), 3, rank).reshape(2, NG, 2, OUTER)
    side = jnp.pad(side, ((0, 0), (0, 0), (0, 0), (0, LANES - OUTER))).reshape(2, NG, 2 * LANES)
    x_fwd = jnp.concatenate([cast(inner(fwd, 3)).reshape(2, NG, 2 * LANES), side], 2)
    side = met(cast(outer(bwd, 1).reshape(2, fft_count, side_share, 2, NG)), 1, rank).reshape(2, OUTER, 2, NG)
    side = jnp.pad(side, ((0, 0), (0, LANES - OUTER), (0, 0), (0, 0))).reshape(2 * LANES, 2, NG)
    x_bwd = jnp.concatenate([cast(inner(bwd, 1)).reshape(2 * LANES, 2, NG), side], 0)
    split = fwd.reshape(2, GROUPS, GROUP, 2, fft_count, share)
    y_fwd = met(cast(split.transpose(4, 3, 5, 0, 2, 1)), 0, rank).reshape(full, full)
    y_fwd_side = cast(inner(fwd.reshape(2, GROUPS, GROUP, 2, NG).transpose(0, 2, 1, 3, 4), 4)).reshape(full, 2 * LANES)
    edges = np.cumsum([0] + chunks)
    spans = list(zip(edges[:-1], edges[1:]))
    z_fwd = fwd.reshape(2, fft_count, share, full).transpose(3, 0, 1, 2)
    z_fwd = met(cast(z_fwd), 2, rank)
    z_fwd = jnp.concatenate([z_fwd[:, :, :, a:b].reshape(full, 2, -1) for a, b in spans], 2).reshape(full, full)
    z_bwd = met(cast(bwd.reshape(2, NG, 2, fft_count, share).transpose(3, 2, 4, 0, 1)), 0, rank)
    z_bwd = jnp.concatenate([z_bwd[:, :, a:b].reshape(-1, full) for a, b in spans], 0)
    order = bwd.reshape(2, NG, 2, GROUPS, GROUP).transpose(2, 4, 3, 0, 1)
    y_bwd = met(cast(order.reshape(full, 2, fft_count, share)), 2, rank).reshape(full, full)
    y_bwd_side = cast(inner(order, 4)).reshape(full, 2 * LANES)
    return x_fwd, x_bwd, y_fwd, y_fwd_side, z_fwd, z_bwd, y_bwd, y_bwd_side


def signed(frequency, grid_size):
    return jnp.where(frequency >= grid_size // 2, frequency - grid_size, frequency)


def kernel_table(column_x, column_y, live, shift_q, grid_size):
    freq_x = signed(column_x, grid_size)
    freq_y = signed(column_y, grid_size)
    freq_z = signed(jnp.arange(grid_size, dtype=jnp.int32), grid_size)
    radius = grid_size // 2
    inside = (freq_x * freq_x + freq_y * freq_y)[None, :] + (freq_z * freq_z)[:, None] <= radius * radius
    inside = jnp.logical_and(inside, live[None, :])
    wave_x = freq_x.astype(jnp.float32) + shift_q[0]
    wave_y = freq_y.astype(jnp.float32) + shift_q[1]
    wave_z = freq_z.astype(jnp.float32) + shift_q[2]
    square = (wave_z * wave_z)[:, None] + (wave_x * wave_x + wave_y * wave_y)[None, :]
    cell = SPACING_BOHR * grid_size
    exponent = math.pi * math.pi * square / (cell * cell * SCREENING * SCREENING)
    weights = cell * cell / math.pi * -jnp.expm1(-exponent) / square / float(grid_size) ** 3
    return jnp.where(inside, weights, 0.0)


def momentum(kpoint_grid, pool_rank, pool_count):
    pool_rows = jnp.arange(pool_count, dtype=jnp.int32)
    earlier = (pool_rank + pool_count - 1) % pool_count
    current = jnp.sum(jnp.where((pool_rows == pool_rank)[:, None], kpoint_grid, 0), axis=0)
    previous = jnp.sum(jnp.where((pool_rows == earlier)[:, None], kpoint_grid, 0), axis=0)
    return (current - previous).astype(jnp.float32) / KMESH


def one_hot(values, wanted):
    return (wanted[:, None] == values[None, :]).astype(jnp.bfloat16)


def column_weights(stick_map, kpoint_grid, fft_rank, share, side_share):
    pool_count = lax.axis_size("pool")
    shift_q = momentum(kpoint_grid, lax.axis_index("pool"), pool_count)
    lanes = jnp.arange(LANES, dtype=jnp.int32)
    inner_freq = jnp.where(lanes < HALF, lanes, lanes + OUTER)
    own_y = fft_rank * share + jnp.arange(share, dtype=jnp.int32)
    own_x = HALF + fft_rank * side_share + jnp.arange(side_share, dtype=jnp.int32)
    column_y = jnp.where(stick_map >= 0, stick_map // NG, -1)
    column_x = jnp.where(stick_map >= 0, stick_map % NG, -1)
    form = (((1,), (1,)), ((), ()))
    main = lax.dot_general(
        one_hot(column_y, own_y), one_hot(column_x, inner_freq), form, preferred_element_type=jnp.float32
    )
    side = lax.dot_general(
        one_hot(column_x, own_x), one_hot(column_y, inner_freq), form, preferred_element_type=jnp.float32
    )
    live = jnp.concatenate([main, side], axis=0).reshape(-1) > 0.5
    place = jnp.arange((share + side_share) * LANES, dtype=jnp.int32)
    row = place // LANES
    lane_freq = jnp.where(place % LANES < HALF, place % LANES, place % LANES + OUTER)
    is_main = row < share
    ids_x = jnp.where(is_main, lane_freq, HALF + fft_rank * side_share + row - share)
    ids_y = jnp.where(is_main, fft_rank * share + row, lane_freq)
    return kernel_table(ids_x, ids_y, live, shift_q, NG)


def dot(left, right, form=(((1,), (0,)), ((), ()))):
    return lax.dot_general(left, right, form, preferred_element_type=jnp.float32)


def pieces(ref, plane, tile, part):
    return ref[pl.ds(plane * ROWS + 2 * tile + part, GROUPS, stride=STEP), :]


def pairs_of(count):
    return [tuple(range(i, min(i + 2, count))) for i in range(0, count, 2)]


def forward_kernel(*refs, planes, fft_count):
    own_ref, recv_ref, x_ref, y_ref, side_ref = refs[:5]
    out_refs = refs[5:-2]
    own_f, recv_f = refs[-2:]
    share = NG // fft_count
    side_share = OUTER // fft_count
    own_f[...] = own_ref[...].astype(jnp.float32)
    recv_f[...] = recv_ref[...].astype(jnp.float32)
    density = []
    for tile in range(TILES):
        real, imag = [], []
        for z in range(planes):
            ro, io = pieces(own_f, z, tile, 0), pieces(own_f, z, tile, 1)
            rr, ir = pieces(recv_f, z, tile, 0), pieces(recv_f, z, tile, 1)
            real.append(rr * ro + ir * io)
            imag.append(rr * io - ir * ro)
        density.append(
            (jnp.concatenate(real, 0).astype(jnp.bfloat16), jnp.concatenate(imag, 0).astype(jnp.bfloat16))
        )
    along_x = []
    for r in range(GROUP):
        left = jnp.concatenate([density[r][0], density[r + 1][0], density[r][1], density[r + 1][1]], axis=1)
        along_x.append(dot(left, x_ref[r]))

    def block(z, r, column):
        return along_x[r][z * GROUPS : (z + 1) * GROUPS, column * LANES : (column + 1) * LANES]

    def stacked(z, first):
        return jnp.concatenate([block(z, r, first + c) for c in range(2) for r in range(GROUP)], axis=0)

    for pair in pairs_of(planes):
        right = jnp.concatenate([stacked(z, 0) for z in pair], axis=1).astype(jnp.bfloat16)
        along_y = dot(y_ref[...], right)
        for n, z in enumerate(pair):
            for k in range(fft_count):
                out_refs[k][z, : 2 * share, :] = along_y[
                    2 * share * k : 2 * share * (k + 1), n * LANES : (n + 1) * LANES
                ].astype(jnp.bfloat16)
    side = stacked(0, 2)
    for z in range(1, planes):
        side = side + pltpu.roll(stacked(z, 2), z * OUTER, 1)
    side = side[:, : planes * OUTER].astype(jnp.bfloat16)
    side_y = dot(side, side_ref[...], (((0,), (0,)), ((), ())))
    for z in range(planes):
        for k in range(fft_count):
            row = z * OUTER + k * side_share
            out_refs[k][z, 2 * share :, :] = jnp.concatenate(
                [side_y[row : row + side_share, c * LANES : (c + 1) * LANES] for c in range(2)], axis=0
            ).astype(jnp.bfloat16)


def column_kernel(*refs, fft_count, chunks):
    count = fft_count * len(chunks)
    in_refs = refs[:count]
    weight_ref, fwd_ref, bwd_ref = refs[count : count + 3]
    out_refs = refs[count + 3 : -1]
    wide = refs[-1]
    share = NG // fft_count
    side_share = OUTER // fft_count
    height = 2 * (share + side_share)
    first = 0
    for in_ref in in_refs:
        rows = in_ref.shape[0] * height
        wide[first : first + rows, :] = in_ref[...].reshape(rows, LANES).astype(jnp.float32)
        first += rows

    def column(i):
        first = i if i < share else 2 * share + i - share
        jump = share if i < share else side_share
        return jnp.concatenate([wide[pl.ds(first + c * jump, NG, stride=height), :] for c in range(2)], axis=0)

    for pair in pairs_of(share + side_share):
        right = jnp.concatenate([column(i) for i in pair], axis=1).astype(jnp.bfloat16)
        spectrum = dot(fwd_ref[...], right)
        weight = weight_ref[:, pair[0] * LANES : (pair[-1] + 1) * LANES]
        scaled = jnp.concatenate([spectrum[:NG] * weight, spectrum[NG:] * weight], axis=0).astype(jnp.bfloat16)
        back = dot(bwd_ref[...], scaled)
        for n, i in enumerate(pair):
            first = 0
            for out_ref in out_refs:
                rows = out_ref.shape[1]
                out_ref[i, :, :] = back[first : first + rows, n * LANES : (n + 1) * LANES].astype(jnp.bfloat16)
                first += rows


def backward_kernel(*refs, planes, depth, fft_count):
    in_refs = refs[:fft_count]
    recv_ref, x_ref, y_ref, side_ref = refs[fft_count : fft_count + 4]
    out_ref, main_f, side_f, recv_f, out_f = refs[-5:]
    share = NG // fft_count
    side_share = OUTER // fft_count
    height = 2 * depth

    @pl.when(pl.program_id(0) == 0)
    def _():
        for k in range(fft_count):
            main_f[k * share * height : (k + 1) * share * height, :] = (
                in_refs[k][:share].reshape(share * height, LANES).astype(jnp.float32)
            )
            side_f[k * side_share * height : (k + 1) * side_share * height, :] = (
                in_refs[k][share:].reshape(side_share * height, LANES).astype(jnp.float32)
            )

    base = pl.program_id(0) * planes
    recv_f[...] = recv_ref[...].astype(jnp.float32)

    def main_of(z):
        return jnp.concatenate(
            [main_f[pl.ds(base + z + c * depth, NG, stride=height), :] for c in range(2)], axis=0
        )

    def side_of(z):
        return jnp.concatenate(
            [side_f[pl.ds(base + z + c * depth, OUTER, stride=height), :] for c in range(2)], axis=1
        )

    back_y = []
    for pair in pairs_of(planes):
        right = jnp.concatenate([main_of(z) for z in pair], axis=1).astype(jnp.bfloat16)
        both = dot(y_ref[...], right)
        back_y += [both[:, n * LANES : (n + 1) * LANES] for n in range(len(pair))]
    packed = jnp.concatenate([side_of(z) for z in range(planes)], axis=0).astype(jnp.bfloat16)
    back_side = dot(side_ref[...], packed, (((1,), (1,)), ((), ())))
    if planes * OUTER < LANES:
        back_side = jnp.concatenate(
            [back_side, jnp.zeros((2 * NG, LANES - planes * OUTER), jnp.float32)], axis=1
        )
    turned = [back_side] + [pltpu.roll(back_side, LANES - z * OUTER, 1) for z in range(1, planes)]
    field = []
    for r in range(GROUP):
        rows = []
        for z in range(planes):
            parts = [v[c * NG + r * GROUPS : c * NG + (r + 1) * GROUPS] for v in (back_y[z], turned[z]) for c in range(2)]
            rows.append(jnp.concatenate(parts, axis=1))
        field.append(dot(jnp.concatenate(rows, axis=0).astype(jnp.bfloat16), x_ref[r]))
    for tile in range(TILES):
        values = []
        for c in range(2):
            value = None
            if tile < GROUP:
                value = field[tile][:, 2 * c * LANES : (2 * c + 1) * LANES]
            if tile > 0:
                late = field[tile - 1][:, (2 * c + 1) * LANES : (2 * c + 2) * LANES]
                value = late if value is None else value + late
            values.append(value)
        for z in range(planes):
            re, im = (v[z * GROUPS : (z + 1) * GROUPS] for v in values)
            rr, ir = pieces(recv_f, z, tile, 0), pieces(recv_f, z, tile, 1)
            out_f[pl.ds(z * ROWS + 2 * tile, GROUPS, stride=STEP), :] = ir * im - rr * re
            out_f[pl.ds(z * ROWS + 2 * tile + 1, GROUPS, stride=STEP), :] = -(rr * im + ir * re)
    out_ref[...] = out_f[...].astype(jnp.bfloat16)


def rows_of(orbitals):
    planes = orbitals.shape[3]
    split = orbitals.reshape(2, planes, NG * NG // LANES, LANES)
    return split.transpose(1, 2, 0, 3).reshape(planes * ROWS, LANES)


def whole(shape):
    return pl.BlockSpec(shape, lambda *_: (0,) * len(shape))


def x_windows(table, axis):
    placed = []
    for r in range(GROUP):
        first = r * (NG - LANES)
        widths = [(0, 0)] * table.ndim
        widths[axis] = (first, 2 * LANES - NG - first)
        placed.append(jnp.pad(table, widths).reshape(4 * LANES, 4 * LANES))
    return jnp.stack(placed)


def exchange(parts):
    count = len(parts)
    moved = [parts[0]]
    for m in range(1, count):
        moved.append(lax.ppermute(parts[m], "fft", [(i, i ^ m) for i in range(count)]))
    return moved


def local(orbitals, stick_map, kpoint_grid):
    planes_all = orbitals.shape[3]
    planes = GROUP if planes_all % GROUP == 0 else 1
    steps = planes_all // planes
    chunk_steps = [steps - steps // 2, steps // 2]
    chunks = [count * planes for count in chunk_steps]
    starts = [0, chunks[0]]
    moved = []
    for a, n in zip(starts, chunks):
        moved.append(shifted(orbitals[:, :, :, a : a + n], "pool", 1))
    fft_count = lax.axis_size("fft")
    fft_rank = lax.axis_index("fft")
    share = NG // fft_count
    side_share = OUTER // fft_count
    columns = share + side_share
    x_fwd, x_bwd, y_fwd, y_fwd_side, z_fwd, z_bwd, y_bwd, y_bwd_side = tables(fft_count, fft_rank, chunks)
    x_fwd = x_windows(x_fwd, 1)
    x_bwd = x_windows(x_bwd, 2)
    weights = column_weights(stick_map, kpoint_grid, fft_rank, share, side_share)
    own = rows_of(orbitals)
    received = [rows_of(piece) for piece in moved]
    block = planes * ROWS
    row_spec = lambda first: pl.BlockSpec((block, LANES), lambda s: (first + s, 0))
    params = pltpu.CompilerParams(vmem_limit_bytes=48 << 20)
    wide = lambda count: pltpu.VMEM((count, LANES), jnp.float32)
    bf16 = lambda *shape: jax.ShapeDtypeStruct(shape, jnp.bfloat16)
    spectra = []
    for c, count in enumerate(chunk_steps):
        spectrum = pl.pallas_call(
            functools.partial(forward_kernel, planes=planes, fft_count=fft_count),
            grid=(count,),
            in_specs=[
                row_spec(starts[c] // planes),
                row_spec(0),
                whole(x_fwd.shape),
                whole(y_fwd.shape),
                whole(y_fwd_side.shape),
            ],
            out_specs=[pl.BlockSpec((planes, 2 * columns, LANES), lambda s: (s, 0, 0))] * fft_count,
            out_shape=[bf16(chunks[c], 2 * columns, LANES)] * fft_count,
            scratch_shapes=[wide(block), wide(block)],
            compiler_params=params,
            name="density_xy",
        )(own, received[c], x_fwd, y_fwd, y_fwd_side)
        spectra += exchange(spectrum)
    scaled = pl.pallas_call(
        functools.partial(column_kernel, fft_count=fft_count, chunks=chunks),
        out_shape=[bf16(columns, 2 * depth, LANES) for depth in chunks for _ in range(fft_count)],
        scratch_shapes=[wide(NG * 2 * columns)],
        compiler_params=params,
        name="columns",
    )(*spectra, weights, z_fwd, z_bwd)
    returned = [exchange(scaled[c * fft_count : (c + 1) * fft_count]) for c in range(len(chunks))]
    result = None
    for c, count in enumerate(chunk_steps):
        inputs = [*returned[c], received[c], x_bwd, y_bwd, y_bwd_side]
        specs = [whole(piece.shape) for piece in returned[c]]
        specs += [row_spec(0), whole(x_bwd.shape), whole(y_bwd.shape), whole(y_bwd_side.shape)]
        if c > 0:
            inputs.append(result)
            specs.append(pl.BlockSpec(memory_space=pl.ANY))
        result = pl.pallas_call(
            functools.partial(backward_kernel, planes=planes, depth=chunks[c], fft_count=fft_count),
            grid=(count,),
            in_specs=specs,
            out_specs=row_spec(starts[c] // planes),
            out_shape=bf16(planes_all * ROWS, LANES),
            scratch_shapes=[wide(NG * 2 * chunks[c]), wide(OUTER * 2 * chunks[c]), wide(block), wide(block)],
            input_output_aliases={len(inputs) - 1: 0} if c > 0 else {},
            compiler_params=params,
            name="yx_action",
        )(*inputs)
    result = result.reshape(planes_all, NG * NG // LANES, 2, LANES).transpose(2, 0, 1, 3)
    return result.reshape(orbitals.shape)


def solution(mesh):
    return jax.shard_map(
        local,
        mesh=mesh,
        in_specs=(P("pool", None, None, "fft", None), P(), P()),
        out_specs=P("pool", None, None, "fft", None),
        check_vma=False,
    )
```
